256 devices in a mesh: rel: 2 (over y_hi), row: 8 (over y_lo, x), col: 16 (over z, core).
Axes of the slice: x: 4, y: 4 (y_hi: 2, y_lo: 2; y = y_hi * 2 + y_lo), z: 8, core: 2. Of those that a mesh axis runs over, the one named last changes fastest.
Arguments:
- features: float32 [4, 128, 256, 128], P('rel', ('row', 'col')), may hold values from -6 to 6
- lap_tiles: bfloat16 [4, 8, 16, 16, 256, 256], P('rel', 'row', 'col'), may hold values from -0.046875 to 0.046875
- tile_rows: int32 [4, 8, 16, 16], P('rel', 'row', 'col'), may hold values from 0 to 15
- tile_cols: int32 [4, 8, 16, 16], P('rel', 'row', 'col'), may hold values from 0 to 7
- tile_count: int32 [4, 8, 16], P('rel', 'row', 'col'), may hold values from 2 to 16, as said below
- cheb_coefs: float32 [4, 5], P('rel'), may hold values from -1 to 1
- merging_weight: bfloat16 [512, 128], replicated, may hold values from -0.25 to 0.25
Outputs:
- merged_rows: float32 [128, 256, 128], P(('row', 'col'), 'rel')
The draws below stay inside these ranges and needn't reach their ends.
Inputs may be any that keep to these rules, and one draw needn't show every extreme that they name: Only the first tile_count slots of a device count; in every relation some device has 16 valid slots.
All inputs are finite; a program needn't handle non-finite values.
Results may differ from the reference program's by a relative error of at most 0.0063.
Values may be sent and summed in bfloat16 or wider, within the bound.
A program may use at most 64 MiB of HBM per device.

```python
import jax
import jax.numpy as jnp
from jax import lax

D = 128
TILE = 256
ORDERS = 4
PB = 1
TPD = 16
RELS = 4
PIECES = 128
PIECE_ROWS = 256
BLOCKS = 128
N_ROW = 8
N_COL = 16


def draw_tile_count(key, part):
    shift_key, pick_key = jax.random.split(key)
    levels = jnp.array([TPD, TPD // 2, TPD // 4, TPD // 8], dtype=jnp.int32)
    shifts = jax.random.randint(shift_key, (RELS, N_ROW * N_COL), 0, 4)
    counts = levels[shifts]
    chosen = jax.random.randint(pick_key, (RELS, 1), 0, N_ROW * N_COL)
    counts = jnp.where(jnp.arange(N_ROW * N_COL, dtype=jnp.int32)[None, :] == chosen, TPD, counts)
    return counts.reshape(RELS, N_ROW, N_COL).astype(jnp.int32)


def plant(drawn, own_key, low, high):
    shape = drawn.shape
    index_at = [jax.random.randint(jax.random.fold_in(own_key, axis), (), 0, shape[axis]) for axis in range(len(shape))]
    drawn = drawn.at[tuple(index_at)].set(low)
    longest = shape.index(max(shape))
    index_at[longest] = (index_at[longest] + 1) % shape[longest]
    return drawn.at[tuple(index_at)].set(high)


def block_levels(key, extent, shards, low, high):
    loudness = 1.0
    for dim, shards_of in shards:
        heights = jax.random.uniform(jax.random.fold_in(jax.random.fold_in(key, 6), dim), (shards_of,), jnp.float32, low / len(shards), high / len(shards))
        loudness = loudness * jnp.repeat(jnp.exp(heights), extent[dim] // shards_of).reshape((-1,) + (1,) * (len(extent) - 1 - dim))
    return loudness


def normal_values(stream_key, extent, deviation, bound, cuts=(), kind=jnp.bfloat16):
    level = block_levels(stream_key, extent, cuts, -0.22, 0.18) if cuts else 1.0
    drawn = jax.random.normal(stream_key, extent, jnp.float32) * deviation * level
    return jnp.minimum(jnp.maximum(drawn, -bound), bound).astype(kind)


def setup_inputs(seed: int = 0) -> dict:
    key_list = jax.random.split(jax.random.key(seed), 8)
    return {
        "features": normal_values(key_list[0], (RELS, PIECES, PIECE_ROWS, D), 1.0, 6.0, ((0, 2), (1, 128)), jnp.float32),
        "lap_tiles": normal_values(key_list[1], (RELS, N_ROW, N_COL, TPD, TILE, TILE), (4 * TILE * TPD // PB) ** -0.5, 0.046875, ((0, 2), (1, 8), (2, 16))),
        "tile_rows": plant(jax.random.randint(key_list[2], (RELS, N_ROW, N_COL, TPD), 0, N_COL * PB), jax.random.fold_in(key_list[2], 1), 0, (N_COL * PB) - 1).astype(jnp.int32),
        "tile_cols": plant(jax.random.randint(key_list[3], (RELS, N_ROW, N_COL, TPD), 0, N_ROW * PB), jax.random.fold_in(key_list[3], 1), 0, (N_ROW * PB) - 1).astype(jnp.int32),
        "tile_count": draw_tile_count(jax.random.fold_in(key_list[7], 71), 0),
        "cheb_coefs": jnp.clip(jax.random.uniform(key_list[5], (RELS, ORDERS + 1), jnp.float32, -1.0, 1.0) * block_levels(key_list[5], (RELS, ORDERS + 1), ((0, 2),), -0.4, 0.0), -1.0, 1.0),
        "merging_weight": normal_values(key_list[6], (RELS * D, D), (RELS * D) ** -0.5, 0.25),
    }


def shard_product(lap_tiles, tile_rows, tile_cols, tile_count, operand):
    blocks = operand.astype(jnp.float32).reshape(BLOCKS, TILE, D)
    col_index = jnp.arange(N_COL, dtype=jnp.int32)[:, None]
    slot_index = jnp.arange(TPD, dtype=jnp.int32)[None, :]

    def one_shard(inputs):
        shard_tiles, shard_rows, shard_cols, shard_count = inputs
        piece_index = (shard_cols // PB) * N_COL + col_index
        global_block = (piece_index * PB + shard_cols % PB).astype(jnp.int32)
        sources = blocks[global_block]
        products = jnp.einsum("cpab,cpbd->cpad", shard_tiles.astype(jnp.float32), sources,
                              precision=lax.Precision.HIGHEST)
        live_mask = (slot_index < shard_count[:, None]).astype(jnp.float32)
        products = products * live_mask[:, :, None, None]
        return jax.ops.segment_sum(products.reshape(N_COL * TPD, TILE, D),
                                   shard_rows.reshape(-1).astype(jnp.int32),
                                   num_segments=N_COL * PB)

    result = lax.map(one_shard, (lap_tiles, tile_rows, tile_cols, tile_count))
    return result.reshape(BLOCKS * TILE, D)


def reference(features, lap_tiles, tile_rows, tile_cols, tile_count, cheb_coefs, merging_weight):
    embeddings = []
    for relation in range(RELS):
        current = features[relation].reshape(BLOCKS * TILE, D)
        earlier = current
        embedding = cheb_coefs[relation, 0] * current
        for degree in range(1, ORDERS + 1):
            applied = shard_product(lap_tiles[relation], tile_rows[relation], tile_cols[relation],
                                    tile_count[relation], current.astype(jnp.bfloat16))
            if degree == 1:
                following = applied
            else:
                following = 2.0 * applied - earlier
            earlier, current = current, following
            embedding = embedding + cheb_coefs[relation, degree] * current
        embeddings.append(embedding.astype(jnp.bfloat16))
    joined = jnp.concatenate(embeddings, axis=1)
    merged_rows = jnp.dot(joined, merging_weight, preferred_element_type=jnp.float32)
    return merged_rows.reshape(PIECES, PIECE_ROWS, D)
```

```python
import functools

import jax
import jax.numpy as jnp
from jax import lax
from jax.experimental import pallas as pl
from jax.experimental.pallas import tpu as pltpu
from jax.sharding import PartitionSpec as P

ORDERS = 4
X_CHIPS = 4
Y_LOW = 2
MESH = pl.DeviceIdType.MESH
ROW_OFFSETS = ((1, 2), (1, 1), (1, 3), (0, 2), (1, 0), (0, 1), (0, 3))
DELTAS = (4, 3, -3, 2, -2, 1, -1, 0)
MIDDLE = 3


def kernel(
    sizes,
    feats,
    tiles,
    rows,
    cols,
    count,
    coefs,
    weight,
    out,
    tiles_v,
    prefix,
    before,
    final,
    hist,
    emb,
    emb_send,
    emb_recv,
    load_sem,
    row_send,
    row_recv,
    pair_send,
    pair_recv,
    ring_send,
    ring_recv,
    rel_send,
    rel_recv,
    *buffers,
):
    rels, slots, blocks, z_count, piece, width = sizes
    half = piece // 2
    per = rels * ORDERS
    gathered = buffers[:per]
    pair_out = buffers[per : 2 * per]
    pair_in = buffers[2 * per : 3 * per]
    ring_out = buffers[3 * per : 4 * per]
    ring_in = buffers[4 * per :]

    rel = lax.axis_index("rel")
    row = lax.axis_index("row")
    col = lax.axis_index("col")
    y, x = row // X_CHIPS, row % X_CHIPS
    z, core = col // 2, col % 2

    def row_peer(dy, dx):
        return ((y + dy) % Y_LOW) * X_CHIPS + (x + dx) % X_CHIPS

    def col_peer(dz):
        return ((z + dz) % z_count) * 2 + core

    partner = z * 2 + (1 - core)
    other_rel = 1 - rel

    loads = [
        pltpu.make_async_copy(tiles.at[l], tiles_v.at[l], load_sem.at[l]) for l in range(rels)
    ]
    for load in loads:
        load.start()

    barrier = pltpu.get_barrier_semaphore()
    for dy, dx in ROW_OFFSETS:
        pl.semaphore_signal(barrier, inc=1, device_id={"row": row_peer(dy, dx)}, device_id_type=MESH)
    for other in (partner, col_peer(1), col_peer(-1)):
        pl.semaphore_signal(barrier, inc=1, device_id={"col": other}, device_id_type=MESH)
    pl.semaphore_signal(barrier, inc=1, device_id={"rel": other_rel}, device_id_type=MESH)

    for l in range(rels):
        start = feats[l]
        hist[l, 0] = start
        emb[l] = coefs[l, 0] * start
        gathered[l * ORDERS][row] = start.astype(jnp.bfloat16)
        prefix[l, slots] = jnp.zeros((piece, width), jnp.float32)
    pl.semaphore_wait(barrier, len(ROW_OFFSETS) + 4)

    sends = []

    def send(copy):
        copy.start()
        sends.append(copy)

    def row_copy(l, k, n, source_row, target):
        buffer = gathered[l * ORDERS + k]
        return pltpu.make_async_remote_copy(
            src_ref=buffer.at[source_row],
            dst_ref=buffer.at[source_row],
            send_sem=row_send.at[l, k, n],
            recv_sem=row_recv.at[l, k, n],
            device_id={"row": target},
            device_id_type=MESH,
        )

    def gather_start(l, k):
        for n, (dy, dx) in enumerate(ROW_OFFSETS):
            send(row_copy(l, k, n, row, row_peer(dy, dx)))

    def gather_wait(l, k):
        for n, (dy, dx) in enumerate(ROW_OFFSETS):
            origin = row_peer(-dy, -dx)
            row_copy(l, k, n, origin, row_peer(dy, dx)).wait_recv()

    def pair_copy(l, k, n):
        at = l * ORDERS + k
        return pltpu.make_async_remote_copy(
            src_ref=pair_out[at].at[n],
            dst_ref=pair_in[at].at[n],
            send_sem=pair_send.at[l, k, n],
            recv_sem=pair_recv.at[l, k, n],
            device_id={"col": partner},
            device_id_type=MESH,
        )

    def multiply(l, k):
        source = gathered[l * ORDERS + k]

        def advance(s, carry):
            product = jnp.dot(
                tiles_v[l, s], source[cols[l, s]], preferred_element_type=jnp.float32
            )
            prefix[l, s] = product + prefix[l, before[l, s]]
            return carry

        lax.fori_loop(0, slots, advance, 0, unroll=4)

    def pair_start(l, k):
        for n, delta in enumerate(DELTAS):
            block = ((z + delta) % z_count) * 2 + (1 - core)
            pair_out[l * ORDERS + k][n] = prefix[l, final[l, block]].astype(jnp.bfloat16)
            send(pair_copy(l, k, n))

    def share(l, k, n, lo, size):
        block = ((z + DELTAS[n]) % z_count) * 2 + core
        own = prefix[l, final[l, block], lo : lo + size]
        return own + pair_in[l * ORDERS + k][n, lo : lo + size].astype(jnp.float32)

    def ring_copy(l, k, side, t, h):
        at = l * ORDERS + k
        return pltpu.make_async_remote_copy(
            src_ref=ring_out[at].at[side, t, pl.ds(h * half, half)],
            dst_ref=ring_in[at].at[side, t, pl.ds(h * half, half)],
            send_sem=ring_send.at[l, k, side, t, h],
            recv_sem=ring_recv.at[l, k, side, t, h],
            device_id={"col": col_peer(1 - 2 * side)},
            device_id_type=MESH,
        )

    def ring_step(l, k, t):
        at = l * ORDERS + k
        numbers = [0, 0] if t == 0 else [2 * t - 1, 2 * t]
        for n in sorted(set(numbers)):
            pair_copy(l, k, n).wait_recv()
        for late in (0, 1):
            if t == 0 and late:
                continue
            for side in (0, 1):
                h = side ^ late
                lo = h * half
                value = share(l, k, numbers[side], lo, half)
                if t > late:
                    ring_copy(l, k, side, t - 1, h).wait_recv()
                    value = value + ring_in[at][side, t - 1, lo : lo + half].astype(jnp.float32)
                ring_out[at][side, t, lo : lo + half] = value.astype(jnp.bfloat16)
                send(ring_copy(l, k, side, t, h))

    def finish(l, k):
        at = l * ORDERS + k
        last = len(DELTAS) - 1
        pair_copy(l, k, last).wait_recv()
        for side in (0, 1):
            for h in (0, 1):
                ring_copy(l, k, side, 3, h).wait_recv()
        applied = (
            share(l, k, last, 0, piece)
            + ring_in[at][0, 3].astype(jnp.float32)
            + ring_in[at][1, 3].astype(jnp.float32)
        )
        if k == 0:
            following = applied
        else:
            following = 2.0 * applied - hist[l, (k + 1) % 2]
        if k + 1 < ORDERS:
            gathered[at + 1][row] = following.astype(jnp.bfloat16)
            gather_start(l, k + 1)
            hist[l, (k + 1) % 2] = following
            emb[l] = emb[l] + coefs[l, k + 1] * following
        else:
            emb_send[l] = (emb[l] + coefs[l, k + 1] * following).astype(jnp.bfloat16)
            send(rel_copy(l))

    def rel_copy(l):
        there = pl.ds(pl.multiple_of(other_rel * half, half), half)
        return pltpu.make_async_remote_copy(
            src_ref=emb_send.at[l, there],
            dst_ref=emb_recv.at[l],
            send_sem=rel_send.at[l],
            recv_sem=rel_recv.at[l],
            device_id={"rel": other_rel},
            device_id_type=MESH,
        )

    for l in range(rels):
        gather_start(l, 0)

    for l in range(rels):
        live = count[l]

        def fill_before(s, carry, l=l, live=live):
            mine = rows[l, s]
            prev = jnp.int32(slots)
            for t in range(slots):
                same = (rows[l, t] == mine) & (t < s) & (t < live)
                prev = jnp.where(same, jnp.int32(t), prev)
            before[l, s] = prev
            return carry

        def fill_final(b, carry, l=l, live=live):
            last = jnp.int32(slots)
            for t in range(slots):
                same = (rows[l, t] == b) & (t < live)
                last = jnp.where(same, jnp.int32(t), last)
            final[l, b] = last
            return carry

        lax.fori_loop(0, slots, fill_before, 0)
        lax.fori_loop(0, blocks, fill_final, 0)

    def product(l, k):
        gather_wait(l, k)
        if k == 0:
            loads[l].wait()
        multiply(l, k)
        pair_start(l, k)

    work = [(l, k) for k in range(ORDERS) for l in range(rels)]
    product(*work[0])
    for index, (l, k) in enumerate(work):
        for t in range(4):
            ring_step(l, k, t)
            if t == MIDDLE - 1 and index + 1 < len(work):
                product(*work[index + 1])
        finish(l, k)

    total = jnp.zeros((half, width), jnp.float32)
    here = pl.ds(pl.multiple_of(rel * half, half), half)
    for l in range(rels):
        own_rows = pl.ds(pl.multiple_of((rel * rels + l) * width, width), width)
        total = total + jnp.dot(
            emb_send[l, here], weight[own_rows], preferred_element_type=jnp.float32
        )
    for l in range(rels):
        rel_copy(l).wait_recv()
        far_rows = pl.ds(pl.multiple_of((other_rel * rels + l) * width, width), width)
        total = total + jnp.dot(
            emb_recv[l], weight[far_rows], preferred_element_type=jnp.float32
        )
    out[...] = total
    for copy in sends:
        copy.wait_send()


def local(features, lap_tiles, tile_rows, tile_cols, tile_count, cheb_coefs, merging_weight):
    rels, _, piece, width = features.shape
    slots, side = lap_tiles.shape[3], lap_tiles.shape[4]
    row_count, blocks = lax.axis_size("row"), lax.axis_size("col")
    z_count = blocks // 2
    sizes = (rels, slots, blocks, z_count, piece, width)
    half = piece // 2
    per = rels * ORDERS
    vmem = functools.partial(pltpu.VMEM, dtype=jnp.bfloat16)
    dma = pltpu.SemaphoreType.DMA
    smem = pl.BlockSpec(memory_space=pltpu.SMEM)
    dense = pl.BlockSpec(memory_space=pltpu.VMEM)
    merged = pl.pallas_call(
        functools.partial(kernel, sizes),
        out_shape=jax.ShapeDtypeStruct((half, width), jnp.float32),
        in_specs=[dense, pl.BlockSpec(memory_space=pltpu.HBM), smem, smem, smem, smem, dense],
        out_specs=dense,
        scratch_shapes=[
            vmem((rels, slots, side, side)),
            pltpu.VMEM((rels, slots + 1, piece, width), jnp.float32),
            pltpu.SMEM((rels, slots), jnp.int32),
            pltpu.SMEM((rels, blocks), jnp.int32),
            pltpu.VMEM((rels, 2, piece, width), jnp.float32),
            pltpu.VMEM((rels, piece, width), jnp.float32),
            vmem((rels, piece, width)),
            vmem((rels, half, width)),
            dma((rels,)),
            dma((rels, ORDERS, row_count - 1)),
            dma((rels, ORDERS, row_count - 1)),
            dma((rels, ORDERS, z_count)),
            dma((rels, ORDERS, z_count)),
            dma((rels, ORDERS, 2, 4, 2)),
            dma((rels, ORDERS, 2, 4, 2)),
            dma((rels,)),
            dma((rels,)),
        ]
        + [vmem((row_count, piece, width))] * per
        + [vmem((z_count, piece, width))] * (2 * per)
        + [vmem((2, 4, piece, width))] * (2 * per),
        compiler_params=pltpu.CompilerParams(
            collective_id=0, has_side_effects=True, vmem_limit_bytes=56 * 1024 * 1024
        ),
    )(
        features[:, 0],
        lap_tiles[:, 0, 0],
        tile_rows[:, 0, 0],
        tile_cols[:, 0, 0],
        tile_count[:, 0, 0],
        cheb_coefs,
        merging_weight,
    )
    return merged[None]


def solution(mesh):
    placed = (
        P("rel", ("row", "col"), None, None),
        P("rel", "row", "col", None, None, None),
        P("rel", "row", "col", None),
        P("rel", "row", "col", None),
        P("rel", "row", "col"),
        P("rel", None),
        P(),
    )
    return jax.shard_map(
        local, mesh=mesh, in_specs=placed, out_specs=P(("row", "col"), "rel", None), check_vma=False
    )
```

```python
import functools

import jax
import jax.numpy as jnp
from jax import lax
from jax.experimental import pallas as pl
from jax.experimental.pallas import tpu as pltpu
from jax.sharding import PartitionSpec as P

ORDERS = 4
X_CHIPS = 4
Y_LOW = 2
MESH = pl.DeviceIdType.MESH
ROW_OFFSETS = ((1, 2), (1, 1), (1, 3), (0, 2), (1, 0), (0, 1), (0, 3), (0, 0))
DELTAS = (3, -3, 4, 2, -2, 1, -1, 0)
ENDS = (0, 1)
HALVES = (0, 1)
SIDES = (0, 1)
UNROLL = 8


def kernel(
    sizes,
    feats,
    tiles,
    table,
    table_out,
    coefs,
    weight,
    out,
    tiles_v,
    far_table,
    prefix,
    sources,
    before,
    final,
    hist,
    emb,
    emb_send,
    emb_recv,
    emb_own,
    start_sem,
    tile_sem,
    tile_send,
    tile_recv,
    table_sems,
    hist_send,
    hist_recv,
    row_send,
    row_recv,
    sum_send,
    sum_recv,
    relay_send,
    relay_recv,
    rel_send,
    rel_recv,
    *buffers,
):
    rels, slots, blocks, z_count, piece, width = sizes
    half = piece // 2
    per = rels * ORDERS
    gathered = buffers[: 2 * per]
    operand = buffers[2 * per : 3 * per]
    sums_out = buffers[3 * per : 4 * per]
    sums_in = buffers[4 * per : 5 * per]
    relay_out = buffers[5 * per : 6 * per]
    relay_in = buffers[6 * per :]
    f32, bf16 = jnp.float32, jnp.bfloat16

    rel = lax.axis_index("rel")
    row = lax.axis_index("row")
    col = lax.axis_index("col")
    y, x = row // X_CHIPS, row % X_CHIPS
    z, core = col // 2, col % 2
    other_rel = 1 - rel
    comm = core == 1
    comp = core == 0

    row_peers = {
        (dy, dx): ((y + dy) % Y_LOW) * X_CHIPS + (x + dx) % X_CHIPS
        for dy in (-1, 0, 1)
        for dx in range(-3, 4)
    }
    chips = {dz: (z + dz) % z_count for dz in range(-4, 5)}

    def row_peer(dy, dx):
        return row_peers[dy, dx]

    def ring_peer(dz, end):
        return chips[dz] * 2 + end

    def at_device(rel=rel, row=row, col=col):
        return (rel, row, col)

    def remote(src, dst, send_sem, recv_sem, **device):
        return pltpu.make_async_remote_copy(
            src_ref=src,
            dst_ref=dst,
            send_sem=send_sem,
            recv_sem=recv_sem,
            device_id=at_device(**device),
            device_id_type=MESH,
        )

    started = {"comm": [], "comp": []}

    def send(who, make, *args):
        make(*args).start()
        started[who].append((make, args))

    def tile_load(l):
        return pltpu.make_async_copy(tiles.at[l], tiles_v.at[l, 0], tile_sem.at[l])

    def tile_copy(l):
        return remote(
            tiles.at[l], tiles_v.at[l, 1], tile_send.at[l], tile_recv.at[l], col=ring_peer(0, 0)
        )

    def table_copy():
        return remote(
            table_out, far_table, table_sems.at[0], table_sems.at[1], col=ring_peer(0, 0)
        )

    def feature_load(l):
        return pltpu.make_async_copy(feats.at[l], hist.at[l, 0, 1], start_sem.at[l])

    def hist_copy(l):
        return remote(
            feats.at[l], hist.at[l, 0, 0], hist_send.at[l], hist_recv.at[l], col=ring_peer(0, 1)
        )

    def rows_of(h):
        return pl.ds(h * half, half)

    def row_copy(l, k, end, h, n, source_row, target):
        at = l * ORDERS + k
        return remote(
            operand[at].at[end, rows_of(h)],
            gathered[2 * at + end].at[source_row].at[rows_of(h)],
            row_send.at[l, k, end, h, n],
            row_recv.at[l, k, end, h, n],
            row=target,
            col=ring_peer(0, 0),
        )

    def sum_copy(l, k, n, end, h):
        at, dz = l * ORDERS + k, DELTAS[n]
        hops = {3: 1, -3: -1, 4: 2 - 4 * end, 2: 0, -2: 0, 1: 1, -1: -1, 0: 0}[dz]
        return remote(
            sums_out[at].at[n, end, rows_of(h)],
            sums_in[at].at[n, end, rows_of(h)],
            sum_send.at[l, k, n, end, h],
            sum_recv.at[l, k, n, end, h],
            col=ring_peer(hops, 1),
        )

    def relay_copy(l, k, side, end, h):
        at = l * ORDERS + k
        return remote(
            relay_out[at].at[side, end, rows_of(h)],
            relay_in[at].at[side, end, rows_of(h)],
            relay_send.at[l, k, side, end, h],
            relay_recv.at[l, k, side, end, h],
            col=ring_peer(2 - 4 * side, 1),
        )

    def rel_copy(l, end):
        there = pl.ds(pl.multiple_of(other_rel * half, half), half)
        return remote(
            emb_send.at[l, end].at[there],
            emb_recv.at[l],
            rel_send.at[l, end],
            rel_recv.at[l, 0],
            rel=other_rel,
            col=ring_peer(0, end),
        )

    def own_copy(l):
        here = pl.ds(pl.multiple_of(rel * half, half), half)
        return remote(
            emb_send.at[l, 0].at[here],
            emb_own.at[l],
            rel_send.at[l, 2],
            rel_recv.at[l, 1],
            col=ring_peer(0, 0),
        )

    barrier = pltpu.get_barrier_semaphore()

    def greet(**device):
        pl.semaphore_signal(barrier, inc=1, device_id=at_device(**device), device_id_type=MESH)

    far_rows = ROW_OFFSETS[:-1]
    for dy, dx in far_rows:
        greet(row=row_peer(dy, dx), col=ring_peer(0, 0))
    greet(rel=other_rel, col=ring_peer(0, 1))
    for dz in (2, -2):
        greet(col=ring_peer(dz, 1))

    @pl.when(comm)
    def _():
        greet(col=ring_peer(0, 0))
        for dz in (2, -2, 1, -1):
            greet(col=ring_peer(dz, 0))
        greet(rel=other_rel, col=ring_peer(0, 0))

    @pl.when(comp)
    def _():
        for dy, dx in far_rows:
            greet(row=row_peer(dy, dx), col=ring_peer(0, 1))
        for dz in (0, 1, -1):
            greet(col=ring_peer(dz, 1))

    for l in range(rels):
        feature_load(l).start()

    @pl.when(comp)
    def _():
        for l in range(rels):
            tile_load(l).start()

    for l in range(rels):
        feature_load(l).wait()
        operand[l * ORDERS][core] = hist[l, 0, 1].astype(bf16)

    @pl.when(comp)
    def _():
        for l in range(rels):
            gathered[2 * l * ORDERS][row] = hist[l, 0, 1].astype(bf16)

    pl.semaphore_wait(barrier, 2 * len(far_rows) + 6 - 4 * core)

    def gather_start(who, l, k, end, h):
        for n, (dy, dx) in enumerate(ROW_OFFSETS if who == "comm" else far_rows):
            send(who, row_copy, l, k, end, h, n, row, row_peer(dy, dx))

    def gather_wait(l, k, end):
        own = k == 0 and end == 0
        for h in HALVES:
            for n, (dy, dx) in enumerate(far_rows if own else ROW_OFFSETS):
                origin = row_peer(-dy, -dx)
                row_copy(l, k, end, h, n, origin, row_peer(dy, dx)).wait_recv()

    @pl.when(comm)
    def _():
        send("comm", table_copy)
        for l in range(rels):
            for h in HALVES:
                gather_start("comm", l, 0, 1, h)
            send("comm", tile_copy, l)

    @pl.when(comp)
    def _():
        for l in range(rels):
            for h in HALVES:
                gather_start("comp", l, 0, 0, h)
        for l in range(rels):
            send("comp", hist_copy, l)

    work = [(l, k) for k in range(ORDERS) for l in range(rels)]

    def fill_tables():
        prefix[2 * slots] = jnp.zeros((piece, width), f32)
        table_copy().wait_recv()
        tables = (table, far_table)
        for l in range(rels):
            base = l * 2 * slots
            lives = [tables[e][rels * 2 * slots + l] for e in ENDS]

            def row_at(e, t, base=base):
                return tables[e][base + t]

            def last_with(mine, below, lives=lives, row_at=row_at):
                found = mine * 0 + 2 * slots
                for e in ENDS:
                    for t in range(slots):
                        same = (row_at(e, t) == mine) & (t < lives[e])
                        if below is not None:
                            same = same & (e * slots + t < below)
                        found = found + same.astype(jnp.int32) * (e * slots + t - found)
                return found

            for e in ENDS:

                def fill_before(s, carry, l=l, e=e, row_at=row_at, last_with=last_with, base=base):
                    sources[l, e * slots + s] = tables[e][base + slots + s]
                    before[l, e * slots + s] = last_with(row_at(e, s), e * slots + s)
                    return carry

                lax.fori_loop(0, slots, fill_before, 0)

            def fill_final(b, carry, l=l, last_with=last_with):
                final[l, b] = last_with(b, None)
                return carry

            lax.fori_loop(0, blocks, fill_final, 0)

    def product(l, k):
        at = l * ORDERS + k
        for end in ENDS:
            gather_wait(l, k, end)
            if k == 0:
                (tile_copy(l).wait_recv if end else tile_load(l).wait)()
            source = gathered[2 * at + end]

            def advance(s, carry, end=end, source=source):
                g = end * slots + s
                value = jnp.dot(
                    tiles_v[l, end, s], source[sources[l, g]], preferred_element_type=f32
                )
                prefix[g] = value + prefix[before[l, g]]
                return carry

            lax.fori_loop(0, slots, advance, 0, unroll=UNROLL)

    def sums_start(l, k):
        at = l * ORDERS + k

        def put(dz, end):
            n = DELTAS.index(dz)
            block = chips[dz] * 2 + end
            for h in HALVES:
                lo = h * half
                value = prefix[final[l, block], lo : lo + half]
                sums_out[at][n, end, lo : lo + half] = value.astype(bf16)
                send("comp", sum_copy, l, k, n, end, h)

        for end in ENDS:
            for dz in (3, -3, 4, 2, -2):
                put(dz, end)
        for end in ENDS:
            for dz in (1, -1, 0):
                put(dz, end)

    def taken(l, k, dz, end, h):
        n, lo = DELTAS.index(dz), h * half
        sum_copy(l, k, n, end, h).wait_recv()
        return sums_in[l * ORDERS + k][n, end, lo : lo + half].astype(f32)

    def relay(l, k):
        at = l * ORDERS + k
        for end in ENDS:
            for h in HALVES:
                for side in SIDES if end else SIDES[::-1]:
                    lo, sign = h * half, 1 - 2 * side
                    value = taken(l, k, 2 * sign, end, h) + taken(l, k, 3 * sign, end, h)
                    if end == side:
                        value = value + taken(l, k, 4, end, h)
                    relay_out[at][side, end, lo : lo + half] = value.astype(bf16)
                    send("comm", relay_copy, l, k, side, end, h)

    def finish(l, k):
        at = l * ORDERS + k
        for end in ENDS:
            for h in HALVES:
                lo = h * half
                part = slice(lo, lo + half)
                value = taken(l, k, 0, end, h) + taken(l, k, 1, end, h) + taken(l, k, -1, end, h)
                for side in SIDES:
                    relay_copy(l, k, side, end, h).wait_recv()
                    value = value + relay_in[at][side, end, part].astype(f32)
                if k > 0:
                    value = 2.0 * value - hist[l, (k + 1) % 2, end, part]
                if k + 1 < ORDERS:
                    operand[at + 1][end, part] = value.astype(bf16)
                    gather_start("comm", l, k + 1, end, h)
                    hist[l, (k + 1) % 2, end, part] = value
                    emb[l, end, part] = emb[l, end, part] + coefs[l, k + 1] * value
                else:
                    total = emb[l, end, part] + coefs[l, k + 1] * value
                    emb_send[l, end, part] = total.astype(bf16)
            if k + 1 == ORDERS:
                send("comm", rel_copy, l, end)
                if end == 0:
                    send("comm", own_copy, l)

    @pl.when(comp)
    def _():
        fill_tables()
        for l, k in work:
            product(l, k)
            sums_start(l, k)

    @pl.when(comm)
    def _():
        for l in range(rels):
            hist_copy(l).wait_recv()
            for end in ENDS:
                emb[l, end] = coefs[l, 0] * hist[l, 0, end]
        for l, k in work:
            relay(l, k)
            finish(l, k)
        here = pl.ds(pl.multiple_of(rel * half, half), half)
        for l in range(rels):
            emb_own[l] = emb_send[l, 1, here]

    @pl.when(comp)
    def _():
        for l in range(rels):
            own_copy(l).wait_recv()

    total = jnp.zeros((half, width), f32)
    for l in range(rels):
        rel_copy(l, 0).wait_recv()
        for side_rel, part in ((rel, emb_own), (other_rel, emb_recv)):
            rows = pl.ds(pl.multiple_of((side_rel * rels + l) * width, width), width)
            total = total + jnp.dot(part[l], weight[rows], preferred_element_type=f32)
    out[...] = total

    for who, active in (("comm", comm), ("comp", comp)):

        @pl.when(active)
        def _(who=who):
            for make, args in started[who]:
                make(*args).wait_send()


def local(features, lap_tiles, tile_rows, tile_cols, tile_count, cheb_coefs, merging_weight):
    rels, _, piece, width = features.shape
    slots, side = lap_tiles.shape[3], lap_tiles.shape[4]
    row_count, blocks = lax.axis_size("row"), lax.axis_size("col")
    z_count = blocks // 2
    sizes = (rels, slots, blocks, z_count, piece, width)
    half = piece // 2
    per = rels * ORDERS
    table = jnp.concatenate([tile_rows[:, 0, 0], tile_cols[:, 0, 0]], axis=1).reshape(-1)
    table = jnp.concatenate([table, tile_count[:, 0, 0]])
    table = jnp.pad(table, (0, -table.shape[0] % 128))
    vmem = functools.partial(pltpu.VMEM, dtype=jnp.bfloat16)
    wide = functools.partial(pltpu.VMEM, dtype=jnp.float32)
    dma = pltpu.SemaphoreType.DMA
    smem = pl.BlockSpec(memory_space=pltpu.SMEM)
    dense = pl.BlockSpec(memory_space=pltpu.VMEM)
    far = pl.BlockSpec(memory_space=pltpu.HBM)
    merged = pl.pallas_call(
        functools.partial(kernel, sizes),
        out_shape=jax.ShapeDtypeStruct((half, width), jnp.float32),
        in_specs=[far, far, smem, far, smem, dense],
        out_specs=dense,
        scratch_shapes=[
            vmem((rels, 2, slots, side, side)),
            pltpu.SMEM(table.shape, jnp.int32),
            wide((2 * slots + 1, piece, width)),
            pltpu.SMEM((rels, 2 * slots), jnp.int32),
            pltpu.SMEM((rels, 2 * slots), jnp.int32),
            pltpu.SMEM((rels, blocks), jnp.int32),
            wide((rels, 2, 2, piece, width)),
            wide((rels, 2, piece, width)),
            vmem((rels, 2, piece, width)),
            vmem((rels, half, width)),
            vmem((rels, half, width)),
            dma((rels,)),
            dma((rels,)),
            dma((rels,)),
            dma((rels,)),
            dma((2,)),
            dma((rels,)),
            dma((rels,)),
            dma((rels, ORDERS, 2, 2, row_count)),
            dma((rels, ORDERS, 2, 2, row_count)),
            dma((rels, ORDERS, z_count, 2, 2)),
            dma((rels, ORDERS, z_count, 2, 2)),
            dma((rels, ORDERS, 2, 2, 2)),
            dma((rels, ORDERS, 2, 2, 2)),
            dma((rels, 3)),
            dma((rels, 2)),
        ]
        + [vmem((row_count, piece, width))] * (2 * per)
        + [vmem((2, piece, width))] * per
        + [vmem((z_count, 2, piece, width))] * (2 * per)
        + [vmem((2, 2, piece, width))] * (2 * per),
        compiler_params=pltpu.CompilerParams(
            collective_id=0, has_side_effects=True, vmem_limit_bytes=62 * 1024 * 1024
        ),
    )(
        features[:, 0],
        lap_tiles[:, 0, 0],
        table,
        table,
        cheb_coefs,
        merging_weight,
    )
    return merged[None]


def solution(mesh):
    placed = (
        P("rel", ("row", "col"), None, None),
        P("rel", "row", "col", None, None, None),
        P("rel", "row", "col", None),
        P("rel", "row", "col", None),
        P("rel", "row", "col"),
        P("rel", None),
        P(),
    )
    return jax.shard_map(
        local, mesh=mesh, in_specs=placed, out_specs=P(("row", "col"), "rel", None), check_vma=False
    )
```

```python
import functools

import jax
import jax.numpy as jnp
from jax import lax
from jax.experimental import pallas as pl
from jax.experimental.pallas import tpu as pltpu
from jax.sharding import PartitionSpec as P

ORDERS = 4
X_CHIPS = 4
Y_LOW = 2
MESH = pl.DeviceIdType.MESH
ROW_OFFSETS = ((1, 2), (1, 1), (1, 3), (0, 2), (1, 0), (0, 1), (0, 3), (0, 0))
DELTAS = (3, -3, 4, 2, -2, 1, -1, 0)
ENDS = (0, 1)
HALVES = (0, 1)
SIDES = (0, 1)
UNROLL = 16


def kernel(
    sizes,
    feats,
    tiles,
    tile_rows,
    tile_cols,
    tile_count,
    cheb_coefs,
    merging_weight,
    out,
    tiles_v,
    rows_0,
    rows_1,
    cols_0,
    cols_1,
    count_0,
    count_1,
    coefs,
    weight,
    prefix,
    sources,
    before,
    final,
    hist,
    emb,
    emb_send,
    emb_recv,
    emb_own,
    start_sem,
    tile_sem,
    tile_send,
    tile_recv,
    table_load,
    table_send,
    table_recv,
    late_sem,
    hist_send,
    hist_recv,
    row_send,
    row_recv,
    sum_send,
    sum_recv,
    relay_send,
    relay_recv,
    rel_send,
    rel_recv,
    *buffers,
):
    rels, slots, blocks, z_count, piece, width = sizes
    half = piece // 2
    per = rels * ORDERS
    gathered = buffers[: 2 * per]
    operand = buffers[2 * per : 3 * per]
    sums_out = buffers[3 * per : 4 * per]
    sums_in = buffers[4 * per : 5 * per]
    relay_out = buffers[5 * per : 6 * per]
    relay_in = buffers[6 * per :]
    f32, bf16 = jnp.float32, jnp.bfloat16

    rel = lax.axis_index("rel")
    row = lax.axis_index("row")
    col = lax.axis_index("col")
    y, x = row // X_CHIPS, row % X_CHIPS
    z, core = col // 2, col % 2
    other_rel = 1 - rel
    comm = core == 1
    comp = core == 0

    row_peers = {
        (dy, dx): ((y + dy) % Y_LOW) * X_CHIPS + (x + dx) % X_CHIPS
        for dy in (-1, 0, 1)
        for dx in range(-3, 4)
    }
    chips = {dz: (z + dz) % z_count for dz in range(-4, 5)}

    def row_peer(dy, dx):
        return row_peers[dy, dx]

    def ring_peer(dz, end):
        return chips[dz] * 2 + end

    def at_device(rel=rel, row=row, col=col):
        return (rel, row, col)

    def remote(src, dst, send_sem, recv_sem, **device):
        return pltpu.make_async_remote_copy(
            src_ref=src,
            dst_ref=dst,
            send_sem=send_sem,
            recv_sem=recv_sem,
            device_id=at_device(**device),
            device_id_type=MESH,
        )

    started = {"comm": [], "comp": []}

    def send(who, make, *args):
        make(*args).start()
        started[who].append((make, args))

    def tile_load(l):
        return pltpu.make_async_copy(tiles.at[l], tiles_v.at[l, 0], tile_sem.at[l])

    def tile_copy(l):
        return remote(
            tiles.at[l], tiles_v.at[l, 1], tile_send.at[l], tile_recv.at[l], col=ring_peer(0, 0)
        )

    near_tables = ((tile_rows, rows_0), (tile_cols, cols_0), (tile_count, count_0))
    far_tables = ((tile_rows, rows_1), (tile_cols, cols_1), (tile_count, count_1))

    def table_near(i):
        return pltpu.make_async_copy(*near_tables[i], table_load.at[i])

    def table_copy(i):
        src, dst = far_tables[i]
        return remote(src, dst, table_send.at[i], table_recv.at[i], col=ring_peer(0, 0))

    late_loads = [
        pltpu.make_async_copy(cheb_coefs, coefs, late_sem.at[0]),
        pltpu.make_async_copy(merging_weight, weight, late_sem.at[1]),
    ]

    def feature_load(l):
        return pltpu.make_async_copy(feats.at[l], hist.at[l, 0, 1], start_sem.at[l])

    def hist_copy(l):
        return remote(
            feats.at[l], hist.at[l, 0, 0], hist_send.at[l], hist_recv.at[l], col=ring_peer(0, 1)
        )

    def rows_of(h):
        return pl.ds(h * half, half)

    def row_copy(l, k, end, h, n, source_row, target):
        at = l * ORDERS + k
        return remote(
            operand[at].at[end, rows_of(h)],
            gathered[2 * at + end].at[source_row].at[rows_of(h)],
            row_send.at[l, k, end, h, n],
            row_recv.at[l, k, end, h, n],
            row=target,
            col=ring_peer(0, 0),
        )

    def sum_copy(l, k, n, end, h):
        at, dz = l * ORDERS + k, DELTAS[n]
        hops = {3: 1, -3: -1, 4: 2 - 4 * end, 2: 0, -2: 0, 1: 1, -1: -1, 0: 0}[dz]
        return remote(
            sums_out[at].at[n, end, rows_of(h)],
            sums_in[at].at[n, end, rows_of(h)],
            sum_send.at[l, k, n, end, h],
            sum_recv.at[l, k, n, end, h],
            col=ring_peer(hops, 1),
        )

    def relay_copy(l, k, side, end, h):
        at = l * ORDERS + k
        return remote(
            relay_out[at].at[side, end, rows_of(h)],
            relay_in[at].at[side, end, rows_of(h)],
            relay_send.at[l, k, side, end, h],
            relay_recv.at[l, k, side, end, h],
            col=ring_peer(2 - 4 * side, 1),
        )

    def rel_copy(l, end):
        there = pl.ds(pl.multiple_of(other_rel * half, half), half)
        return remote(
            emb_send.at[l, end].at[there],
            emb_recv.at[l],
            rel_send.at[l, end],
            rel_recv.at[l, 0],
            rel=other_rel,
            col=ring_peer(0, end),
        )

    def own_copy(l):
        here = pl.ds(pl.multiple_of(rel * half, half), half)
        return remote(
            emb_send.at[l, 0].at[here],
            emb_own.at[l],
            rel_send.at[l, 2],
            rel_recv.at[l, 1],
            col=ring_peer(0, 0),
        )

    barrier = pltpu.get_barrier_semaphore()

    def greet(**device):
        pl.semaphore_signal(barrier, inc=1, device_id=at_device(**device), device_id_type=MESH)

    far_rows = ROW_OFFSETS[:-1]
    for dy, dx in far_rows:
        greet(row=row_peer(dy, dx), col=ring_peer(0, 0))
    greet(rel=other_rel, col=ring_peer(0, 1))
    for dz in (2, -2):
        greet(col=ring_peer(dz, 1))

    @pl.when(comm)
    def _():
        greet(col=ring_peer(0, 0))
        for dz in (2, -2, 1, -1):
            greet(col=ring_peer(dz, 0))
        greet(rel=other_rel, col=ring_peer(0, 0))

    @pl.when(comp)
    def _():
        for dy, dx in far_rows:
            greet(row=row_peer(dy, dx), col=ring_peer(0, 1))
        for dz in (0, 1, -1):
            greet(col=ring_peer(dz, 1))

    for l in range(rels):
        feature_load(l).start()

    @pl.when(comp)
    def _():
        for i in range(3):
            table_near(i).start()
        for l in range(rels):
            tile_load(l).start()

    for l in range(rels):
        feature_load(l).wait()
        operand[l * ORDERS][core] = hist[l, 0, 1].astype(bf16)

    @pl.when(comp)
    def _():
        for l in range(rels):
            gathered[2 * l * ORDERS][row] = hist[l, 0, 1].astype(bf16)

    for load in late_loads:
        load.start()
    pl.semaphore_wait(barrier, 2 * len(far_rows) + 6 - 4 * core)

    def gather_start(who, l, k, end, h):
        for n, (dy, dx) in enumerate(ROW_OFFSETS if who == "comm" else far_rows):
            send(who, row_copy, l, k, end, h, n, row, row_peer(dy, dx))

    def gather_wait(l, k, end):
        own = k == 0 and end == 0
        for h in HALVES:
            for n, (dy, dx) in enumerate(far_rows if own else ROW_OFFSETS):
                origin = row_peer(-dy, -dx)
                row_copy(l, k, end, h, n, origin, row_peer(dy, dx)).wait_recv()

    @pl.when(comm)
    def _():
        for i in range(3):
            send("comm", table_copy, i)
        for l in range(rels):
            for h in HALVES:
                gather_start("comm", l, 0, 1, h)
            send("comm", tile_copy, l)

    @pl.when(comp)
    def _():
        for l in range(rels):
            for h in HALVES:
                gather_start("comp", l, 0, 0, h)
        for l in range(rels):
            send("comp", hist_copy, l)

    work = [(l, k) for k in range(ORDERS) for l in range(rels)]

    def fill_tables():
        prefix[2 * slots] = jnp.zeros((piece, width), f32)
        for i in range(3):
            table_near(i).wait()
        for i in range(3):
            table_copy(i).wait_recv()
        for l in range(rels):
            none = count_0[l] * 0 + 2 * slots
            lasts = (none,) * blocks
            for e, (rows_e, cols_e, count_e) in enumerate(
                ((rows_0, cols_0, count_0), (rows_1, cols_1, count_1))
            ):
                live = count_e[l]

                def fill(s, lasts, l=l, e=e, rows_e=rows_e, cols_e=cols_e, live=live, none=none):
                    g = e * slots + s
                    mine = rows_e[l, s]
                    found = none
                    after = []
                    for b in range(blocks):
                        hit = mine == b
                        found = jnp.where(hit, lasts[b], found)
                        after.append(jnp.where(hit & (s < live), g, lasts[b]))
                    sources[l, g] = cols_e[l, s]
                    before[l, g] = found
                    return tuple(after)

                lasts = lax.fori_loop(0, slots, fill, lasts)
            for b in range(blocks):
                final[l, b] = lasts[b]

    def product(l, k):
        at = l * ORDERS + k
        for end in ENDS:
            gather_wait(l, k, end)
            if k == 0:
                (tile_copy(l).wait_recv if end else tile_load(l).wait)()
            source = gathered[2 * at + end]

            def advance(s, carry, end=end, source=source):
                g = end * slots + s
                value = jnp.dot(
                    tiles_v[l, end, s], source[sources[l, g]], preferred_element_type=f32
                )
                prefix[g] = value + prefix[before[l, g]]
                return carry

            lax.fori_loop(0, slots, advance, 0, unroll=UNROLL)

    def sums_start(l, k):
        at = l * ORDERS + k

        def put(dz, end, h):
            n, lo = DELTAS.index(dz), h * half
            block = chips[dz] * 2 + end
            value = prefix[final[l, block], lo : lo + half]
            sums_out[at][n, end, lo : lo + half] = value.astype(bf16)
            send("comp", sum_copy, l, k, n, end, h)

        for hops in ((3, -3, 4, 2, -2), (1, -1, 0)):
            for end in ENDS:
                for h in HALVES:
                    for dz in hops:
                        put(dz, end, h)

    def taken(l, k, dz, end, h):
        n, lo = DELTAS.index(dz), h * half
        sum_copy(l, k, n, end, h).wait_recv()
        return sums_in[l * ORDERS + k][n, end, lo : lo + half].astype(f32)

    def relay(l, k):
        at = l * ORDERS + k
        for end in ENDS:
            for h in HALVES:
                for side in SIDES if end else SIDES[::-1]:
                    lo, sign = h * half, 1 - 2 * side
                    value = taken(l, k, 2 * sign, end, h) + taken(l, k, 3 * sign, end, h)
                    if end == side:
                        value = value + taken(l, k, 4, end, h)
                    relay_out[at][side, end, lo : lo + half] = value.astype(bf16)
                    send("comm", relay_copy, l, k, side, end, h)

    def finish(l, k):
        at = l * ORDERS + k
        for end in ENDS:
            for h in HALVES:
                lo = h * half
                part = slice(lo, lo + half)
                value = taken(l, k, 0, end, h) + taken(l, k, 1, end, h) + taken(l, k, -1, end, h)
                for side in SIDES:
                    relay_copy(l, k, side, end, h).wait_recv()
                    value = value + relay_in[at][side, end, part].astype(f32)
                if k > 0:
                    value = 2.0 * value - hist[l, (k + 1) % 2, end, part]
                if k + 1 < ORDERS:
                    operand[at + 1][end, part] = value.astype(bf16)
                    gather_start("comm", l, k + 1, end, h)
                    hist[l, (k + 1) % 2, end, part] = value
                    emb[l, end, part] = emb[l, end, part] + coefs[l, k + 1] * value
                else:
                    total = emb[l, end, part] + coefs[l, k + 1] * value
                    emb_send[l, end, part] = total.astype(bf16)
            if k + 1 == ORDERS:
                send("comm", rel_copy, l, end)
                if end == 0:
                    send("comm", own_copy, l)

    @pl.when(comp)
    def _():
        fill_tables()
        for l, k in work:
            product(l, k)
            sums_start(l, k)

    @pl.when(comm)
    def _():
        for l in range(rels):
            hist_copy(l).wait_recv()
            if l == 0:
                late_loads[0].wait()
            for end in ENDS:
                emb[l, end] = coefs[l, 0] * hist[l, 0, end]
        for l, k in work:
            relay(l, k)
            finish(l, k)
        here = pl.ds(pl.multiple_of(rel * half, half), half)
        for l in range(rels):
            emb_own[l] = emb_send[l, 1, here]

    @pl.when(comp)
    def _():
        for l in range(rels):
            own_copy(l).wait_recv()
        late_loads[0].wait()

    late_loads[1].wait()
    total = jnp.zeros((half, width), f32)

    def merged(part, l, side_rel):
        rows = pl.ds(pl.multiple_of((side_rel * rels + l) * width, width), width)
        return jnp.dot(part[l], weight[rows], preferred_element_type=f32)

    for l in range(rels):
        total = total + merged(emb_own, l, rel)
    for l in range(rels):
        rel_copy(l, 0).wait_recv()
        total = total + merged(emb_recv, l, other_rel)
    out[...] = total

    for who, active in (("comm", comm), ("comp", comp)):

        @pl.when(active)
        def _(who=who):
            for make, args in started[who]:
                make(*args).wait_send()


def local(features, lap_tiles, tile_rows, tile_cols, tile_count, cheb_coefs, merging_weight):
    rels, _, piece, width = features.shape
    slots, side = lap_tiles.shape[3], lap_tiles.shape[4]
    row_count, blocks = lax.axis_size("row"), lax.axis_size("col")
    z_count = blocks // 2
    sizes = (rels, slots, blocks, z_count, piece, width)
    half = piece // 2
    per = rels * ORDERS
    vmem = functools.partial(pltpu.VMEM, dtype=jnp.bfloat16)
    wide = functools.partial(pltpu.VMEM, dtype=jnp.float32)
    dma = pltpu.SemaphoreType.DMA
    dense = pl.BlockSpec(memory_space=pltpu.VMEM)
    far = pl.BlockSpec(memory_space=pltpu.HBM)
    merged = pl.pallas_call(
        functools.partial(kernel, sizes),
        out_shape=jax.ShapeDtypeStruct((half, width), jnp.float32),
        in_specs=[far] * 7,
        out_specs=dense,
        scratch_shapes=[
            vmem((rels, 2, slots, side, side)),
            pltpu.SMEM((rels, slots), jnp.int32),
            pltpu.SMEM((rels, slots), jnp.int32),
            pltpu.SMEM((rels, slots), jnp.int32),
            pltpu.SMEM((rels, slots), jnp.int32),
            pltpu.SMEM((rels,), jnp.int32),
            pltpu.SMEM((rels,), jnp.int32),
            pltpu.SMEM(cheb_coefs.shape, jnp.float32),
            vmem(merging_weight.shape),
            wide((2 * slots + 1, piece, width)),
            pltpu.SMEM((rels, 2 * slots), jnp.int32),
            pltpu.SMEM((rels, 2 * slots), jnp.int32),
            pltpu.SMEM((rels, blocks), jnp.int32),
            wide((rels, 2, 2, piece, width)),
            wide((rels, 2, piece, width)),
            vmem((rels, 2, piece, width)),
            vmem((rels, half, width)),
            vmem((rels, half, width)),
            dma((rels,)),
            dma((rels,)),
            dma((rels,)),
            dma((rels,)),
            dma((3,)),
            dma((3,)),
            dma((3,)),
            dma((2,)),
            dma((rels,)),
            dma((rels,)),
            dma((rels, ORDERS, 2, 2, row_count)),
            dma((rels, ORDERS, 2, 2, row_count)),
            dma((rels, ORDERS, z_count, 2, 2)),
            dma((rels, ORDERS, z_count, 2, 2)),
            dma((rels, ORDERS, 2, 2, 2)),
            dma((rels, ORDERS, 2, 2, 2)),
            dma((rels, 3)),
            dma((rels, 2)),
        ]
        + [vmem((row_count, piece, width))] * (2 * per)
        + [vmem((2, piece, width))] * per
        + [vmem((z_count, 2, piece, width))] * (2 * per)
        + [vmem((2, 2, piece, width))] * (2 * per),
        compiler_params=pltpu.CompilerParams(
            collective_id=0, has_side_effects=True, vmem_limit_bytes=62 * 1024 * 1024
        ),
    )(
        features[:, 0],
        lap_tiles[:, 0, 0],
        tile_rows[:, 0, 0],
        tile_cols[:, 0, 0],
        tile_count[:, 0, 0],
        cheb_coefs,
        merging_weight,
    )
    return merged[None]


def solution(mesh):
    placed = (
        P("rel", ("row", "col"), None, None),
        P("rel", "row", "col", None, None, None),
        P("rel", "row", "col", None),
        P("rel", "row", "col", None),
        P("rel", "row", "col"),
        P("rel", None),
        P(),
    )
    return jax.shard_map(
        local, mesh=mesh, in_specs=placed, out_specs=P(("row", "col"), "rel", None), check_vma=False
    )
```
